128 devices in a mesh: dp: 8 (over y, core), mp: 16 (over x, z).
Axes of the slice: x: 4, y: 4, z: 4, core: 2. Of those that a mesh axis runs over, the one named last changes fastest.
Arguments:
- emb_grad: float32 [65536, 7168], P('dp', 'mp'), may hold values from -600 to 600
- mtp_grad: float32 [14336, 7168], P('dp', 'mp'), may hold values from -600 to 600
- emb_groups: int32 [64], replicated, may hold values from 0 to 31
- mtp_groups: int32 [32], replicated, may hold values from 0 to 31
- max_rms: float32 [1], replicated, may hold values from 0.5 to 2
Outputs:
- emb_clipped: bfloat16 [65536, 7168], P(('dp', 'mp'))
- mtp_clipped: bfloat16 [14336, 7168], P('dp', 'mp')
- group_rms: float32 [32], replicated
The draws below stay inside these ranges and needn't reach their ends.
All inputs are finite; a program needn't handle non-finite values.
Results may differ from the reference program's by a relative error of at most 0.005.
Values may be sent and summed in bfloat16 or wider, within the bound.
No kernel may reach another device: no remote copies, remote signals or barrier semaphores. Data moves between devices by JAX's collectives and lax.ppermute only.
A program may use at most 128 MiB of HBM per device.

```python
import math
import jax
import jax.numpy as jnp
from jax import lax

D = 7168
V = 65536
CAT = 14336
EMB_BLK = 1024
MTP_BLK = 448
GROUPS = 32
EMB_BLOCKS = 64
MTP_BLOCKS = 32


def scaled_gradient(key, height, breadth):
    keys = jax.random.split(key, 3)
    row_pos = jnp.arange(height, dtype=jnp.float32) / height
    col_pos = jnp.arange(breadth, dtype=jnp.float32) / breadth
    lower, upper = (math.log(0.3), math.log(3.0))
    base = jnp.clip(jax.random.normal(keys[0], (height, breadth), jnp.float32), -6.0, 6.0)
    row_scale = 3.0 ** (1.0 - row_pos) * jnp.exp(jax.random.uniform(keys[1], (height,), jnp.float32, lower, upper))
    col_scale = 1.8 ** col_pos * jnp.exp(jax.random.uniform(keys[2], (breadth,), jnp.float32, lower, upper))
    return base * row_scale[:, None] * col_scale[None, :]


def draw_emb_grad(key, part):
    return scaled_gradient(jax.random.fold_in(key, 11), V, D)


def draw_mtp_grad(key, part):
    return scaled_gradient(jax.random.fold_in(key, 23), CAT, D)


def with_ends(result, rng, low, largest):
    dims = result.shape
    index_at = [jax.random.randint(jax.random.fold_in(rng, axis), (), 0, dims[axis]) for axis in range(len(dims))]
    result = result.at[tuple(index_at)].set(low)
    longest = dims.index(max(dims))
    index_at[longest] = (index_at[longest] + 1) % dims[longest]
    return result.at[tuple(index_at)].set(largest)


def setup_inputs(seed: int = 0) -> dict:
    key_of = jax.random.split(jax.random.key(seed), 6)
    emb_grad = draw_emb_grad(jax.random.fold_in(key_of[5], 71), 0)
    mtp_grad = draw_mtp_grad(jax.random.fold_in(key_of[5], 71), 0)
    emb_groups = with_ends(jax.random.randint(key_of[2], (EMB_BLOCKS,), 0, GROUPS), jax.random.fold_in(key_of[2], 1), 0, GROUPS - 1).astype(jnp.int32)
    mtp_groups = with_ends(jax.random.randint(key_of[3], (MTP_BLOCKS,), 0, GROUPS), jax.random.fold_in(key_of[3], 1), 0, GROUPS - 1).astype(jnp.int32)
    max_rms = jnp.clip(jnp.exp(jax.random.uniform(key_of[4], (1,), jnp.float32, math.log(0.5), math.log(2.0))), 0.5, 2.0)
    return dict(emb_grad=emb_grad, mtp_grad=mtp_grad, emb_groups=emb_groups, mtp_groups=mtp_groups, max_rms=max_rms)


def block_squares(gradient, block_rows):
    blocks = gradient.reshape(gradient.shape[0] // block_rows, block_rows, gradient.shape[1])
    return lax.optimization_barrier(jnp.sum(jnp.square(blocks), axis=(1, 2)))

def membership(labels):
    return (labels[:, None] == jnp.arange(GROUPS, dtype=jnp.int32)[None, :]).astype(jnp.float32)

def reference(emb_grad, mtp_grad, emb_groups, mtp_groups, max_rms):
    embed_member = membership(emb_groups)
    head_member = membership(mtp_groups)
    embed_squares = block_squares(emb_grad, EMB_BLK)
    head_squares = block_squares(mtp_grad, MTP_BLK)
    group_square = lax.optimization_barrier(jnp.sum(embed_squares[:, None] * embed_member, axis=0)) + lax.optimization_barrier(jnp.sum(head_squares[:, None] * head_member, axis=0))
    group_size = lax.optimization_barrier(jnp.sum(embed_member, axis=0)) * jnp.float32(EMB_BLK * D) + lax.optimization_barrier(jnp.sum(head_member, axis=0)) * jnp.float32(MTP_BLK * D)
    group_rms = jnp.sqrt(group_square / jnp.maximum(group_size, 1.0))
    global_norm = jnp.sqrt(jnp.sum(group_square))
    ceiling = max_rms[0] * jnp.sqrt(jnp.float32((V + CAT) * D))
    factor = ceiling / (global_norm + 1e-06)
    emb_low = lax.optimization_barrier(emb_grad.astype(jnp.bfloat16))
    emb_clipped = (emb_low.astype(jnp.float32) * factor).astype(jnp.bfloat16)
    mtp_clipped = (mtp_grad * factor).astype(jnp.bfloat16)
    return (emb_clipped, mtp_clipped, group_rms)
```

```python
import jax
import jax.numpy as jnp
from jax import lax
from jax.experimental import pallas as pl
from jax.experimental.pallas import tpu as pltpu
from jax.sharding import Mesh
from jax.sharding import PartitionSpec as P

D = 7168
V = 65536
CAT = 14336
EMB_BLK = 1024
MTP_BLK = 448
GROUPS = 32
DP = ("dp_0", "dp_1")
DP_MP = ("dp_0", "dp_1", "mp_0", "mp_1")
MP = ("mp_0", "mp_1")
PEERS = 16
FEAT = 448
OWN = 512
EXTRA = 16
F32 = jnp.float32
BF16 = jnp.bfloat16
VMEM_LIMIT = 48 * 1024 * 1024


def membership(labels):
    return (labels[:, None] == jnp.arange(GROUPS, dtype=jnp.int32)[None, :]).astype(F32)


def fold_squares(x):
    s = x * x
    t = jnp.sum(s.reshape(FEAT // 8, 8, s.shape[1]), axis=0)
    r = t[:, :128]
    for i in range(1, s.shape[1] // 128):
        r = r + t[:, 128 * i : 128 * (i + 1)]
    return r


def first_kernel(x_ref, piece_ref, acc_ref):
    x = x_ref[...]
    piece_ref[0] = x.astype(BF16)
    acc_ref[0] = fold_squares(x)


def first_pass(grad_t, rows):
    return pl.pallas_call(
        first_kernel,
        grid=(PEERS,),
        in_specs=[pl.BlockSpec((FEAT, rows), lambda p: (0, p * (OWN // rows)))],
        out_specs=[
            pl.BlockSpec((1, FEAT, rows), lambda p: (p, 0, 0)),
            pl.BlockSpec((1, 8, 128), lambda p: (p, 0, 0)),
        ],
        out_shape=[
            jax.ShapeDtypeStruct((PEERS, FEAT, rows), BF16),
            jax.ShapeDtypeStruct((PEERS, 8, 128), F32),
        ],
        compiler_params=pltpu.CompilerParams(vmem_limit_bytes=VMEM_LIMIT),
        name="first_pass",
    )(grad_t)


def second_kernel(labels_ref, xa_ref, xb_ref, m_ref, acc0_ref, mid_ref, last_ref, acc_ref, macc_ref):
    p = pl.program_id(0)
    xa = xa_ref[...]
    xb = xb_ref[...]
    mid_ref[p, :FEAT, :] = xa.astype(BF16)
    last_ref[0] = xb.astype(BF16)
    acc_ref[p] = acc0_ref[0] + fold_squares(xa) + fold_squares(xb)

    @pl.when(p == 0)
    def _():
        macc_ref[...] = jnp.zeros_like(macc_ref)

    @pl.when(p % 2 == 0)
    def _():
        m = m_ref[...]
        macc_ref[...] += jnp.sum((m * m).reshape(m.shape[0] // 8, 8, m.shape[1]), axis=0)

    @pl.when(p == PEERS - 1)
    def _():
        lane = lax.broadcasted_iota(jnp.int32, (8, 128), 1)
        total = jnp.zeros((8, 128), F32)
        for b in range(PEERS // 2):
            s = jnp.sum(acc_ref[2 * b] + acc_ref[2 * b + 1])
            total = total + jnp.where(lane == labels_ref[b], s, 0.0)
        col = lax.broadcasted_iota(jnp.int32, macc_ref.shape, 1)
        for b in range(4):
            s = jnp.sum(jnp.where((col >= MTP_BLK * b) & (col < MTP_BLK * (b + 1)), macc_ref[...], 0.0))
            total = total + jnp.where(lane == labels_ref[8 + b], s, 0.0)
        high = total.astype(BF16).astype(F32)
        middle = (total - high).astype(BF16).astype(F32)
        low = total - high - middle
        row = lax.broadcasted_iota(jnp.int32, (8, 128), 0)
        parts = jnp.where(row == 0, high, jnp.where(row == 1, middle, jnp.where(row == 2, low, 0.0)))
        parts = jnp.concatenate([parts, jnp.zeros((8, 128), F32)], axis=0).astype(BF16)
        for q in range(PEERS):
            mid_ref[q, FEAT:, :] = parts


def second_pass(grad_t, mtp_t, labels, acc0):
    return pl.pallas_call(
        second_kernel,
        grid_spec=pltpu.PrefetchScalarGridSpec(
            num_scalar_prefetch=1,
            grid=(PEERS,),
            in_specs=[
                pl.BlockSpec((FEAT, 128), lambda p, l: (0, 4 * p + 1)),
                pl.BlockSpec((FEAT, 256), lambda p, l: (0, 2 * p + 1)),
                pl.BlockSpec((56, 1792), lambda p, l: (p // 2, 0)),
                pl.BlockSpec((1, 8, 128), lambda p, l: (p, 0, 0)),
            ],
            out_specs=[
                pl.BlockSpec((PEERS, FEAT + EXTRA, 128), lambda p, l: (0, 0, 0)),
                pl.BlockSpec((1, FEAT, 256), lambda p, l: (p, 0, 0)),
            ],
            scratch_shapes=[pltpu.VMEM((PEERS, 8, 128), F32), pltpu.VMEM((8, 1792), F32)],
        ),
        out_shape=[
            jax.ShapeDtypeStruct((PEERS, FEAT + EXTRA, 128), BF16),
            jax.ShapeDtypeStruct((PEERS, FEAT, 256), BF16),
        ],
        compiler_params=pltpu.CompilerParams(vmem_limit_bytes=VMEM_LIMIT),
        name="second_pass",
    )(labels, grad_t, grad_t, mtp_t, acc0)


def place_kernel(factor_ref, x_ref, *rest):
    out_ref = rest[-1]
    x = x_ref[:, :FEAT, :].astype(F32)
    out_ref[...] = (x.reshape(2 * FEAT, x.shape[2]).T * factor_ref[0]).astype(BF16)


def place(factor, received, base, start):
    peers, feat, rows = received.shape
    specs = [
        pl.BlockSpec(memory_space=pltpu.SMEM),
        pl.BlockSpec((2, feat, rows), lambda j: (j, 0, 0)),
    ]
    args = [factor, received]
    alias = {}
    if base is not None:
        specs.append(pl.BlockSpec(memory_space=pl.ANY))
        args.append(base)
        alias = {2: 0}
    return pl.pallas_call(
        place_kernel,
        grid=(PEERS // 2,),
        in_specs=specs,
        out_specs=pl.BlockSpec((rows, 2 * FEAT), lambda j: (start // rows, j)),
        out_shape=jax.ShapeDtypeStruct((OWN, D), BF16),
        input_output_aliases=alias,
        compiler_params=pltpu.CompilerParams(vmem_limit_bytes=VMEM_LIMIT),
        name="place",
    )(*args)


def exchange(pieces):
    return lax.all_to_all(pieces, MP, split_axis=0, concat_axis=0, tiled=True)


def on_device(emb_grad, mtp_grad, emb_groups, mtp_groups, max_rms):
    shard = lax.axis_index(DP)
    labels = jnp.concatenate(
        [
            lax.dynamic_slice_in_dim(emb_groups, shard * 8, 8),
            lax.dynamic_slice_in_dim(mtp_groups, shard * 4, 4),
        ]
    )
    grad_t = emb_grad.T
    mtp_t = mtp_grad.T
    p0, acc0 = first_pass(grad_t, 128)
    r0 = exchange(p0)
    p1, p2 = second_pass(grad_t, mtp_t, labels, acc0)
    r1 = exchange(p1)
    r2 = exchange(p2)
    group_square = jnp.sum(r1[:, FEAT : FEAT + 3, :GROUPS].astype(F32), axis=(0, 1))
    for axis in DP:
        group_square = lax.psum(group_square, axis)
    group_size = jnp.sum(membership(emb_groups), axis=0) * F32(EMB_BLK * D) + jnp.sum(
        membership(mtp_groups), axis=0
    ) * F32(MTP_BLK * D)
    group_rms = jnp.sqrt(group_square / jnp.maximum(group_size, 1.0))
    global_norm = jnp.sqrt(jnp.sum(group_square))
    ceiling = max_rms[0] * jnp.sqrt(F32((V + CAT) * D))
    factor = ceiling / (global_norm + 1e-06)
    head_output = (mtp_grad * factor).astype(BF16)
    scale = factor.reshape(1)
    out = place(scale, r0, None, 0)
    out = place(scale, r1, out, 128)
    out = place(scale, r2, out, 256)
    return (out, head_output, group_rms)


def solution(mesh):
    torus = Mesh(mesh.devices.reshape(4, 2, 4, 4), ("dp_0", "dp_1", "mp_0", "mp_1"))
    return jax.shard_map(
        on_device,
        mesh=torus,
        in_specs=(P(DP, MP), P(DP, MP), P(), P(), P()),
        out_specs=(P(DP_MP, None), P(DP, MP), P()),
        check_vma=False,
    )
```
